512 devices in a mesh: frames: 128 (over x, y_hi, z), heads: 4 (over y_lo, core).
Axes of the slice: x: 4, y: 8 (y_hi: 4, y_lo: 2; y = y_hi * 2 + y_lo), z: 8, core: 2. Of those that a mesh axis runs over, the one named last changes fastest.
Arguments:
- queries: bfloat16 [16384, 4096], P('frames', 'heads'), may hold values from -9 to 9
- keys: bfloat16 [16384, 512], P(('frames', 'heads')), may hold values from -4.5 to 4.5
- values: bfloat16 [16384, 512], P(('frames', 'heads')), may hold values from -6 to 6
- block_mask: int32 [128, 128], replicated, may hold values from 0 to 1, as said below
- lengths: int32 [128], replicated, may hold values from 64 to 128, as said below
Outputs:
- attended: bfloat16 [16384, 4096], P('frames', 'heads')
The draws below stay inside these ranges and needn't reach their ends.
Inputs may be any that keep to these rules, and one draw needn't show every extreme that they name: block_mask[i, i] = 1 and block_mask[i, j] = 0 for j > i. `lengths`: some frame group is full in every draw.
All inputs are finite; a program needn't handle non-finite values.
Results may differ from the reference program's by a relative error of at most 0.0055.
Values may be sent and summed in bfloat16 or wider, within the bound.
No kernel may reach another device: no remote copies, remote signals or barrier semaphores. Data moves between devices by JAX's collectives and lax.ppermute only.
A program may use at most 64 MiB of HBM per device.

```python
import jax
import jax.numpy as jnp
from jax import lax

HEAD_DIM = 128
Q_HEADS = 32
KV_HEADS = 4
TOK_DEV = 128
GROUPS = 128
TOKENS = 16384


def draw_keys(key, part):
    base = jnp.clip(jax.random.normal(jax.random.fold_in(key, 11), (TOKENS, KV_HEADS * HEAD_DIM), jnp.float32), -4.5, 4.5)
    return base.astype(jnp.bfloat16)


def draw_queries(key, part):
    base = jnp.clip(jax.random.normal(jax.random.fold_in(key, 13), (TOKENS, Q_HEADS * HEAD_DIM), jnp.float32), -4.5, 4.5)
    return base.astype(jnp.bfloat16)


def draw_block_mask(key, part):
    draws = jax.random.randint(jax.random.fold_in(key, 19), (GROUPS, GROUPS), 0, 5)
    rows = jnp.arange(GROUPS, dtype=jnp.int32)[:, None]
    cols = jnp.arange(GROUPS, dtype=jnp.int32)[None, :]
    below = (rows > cols) & (draws < 3)
    return jnp.where(below | (rows == cols), 1, 0).astype(jnp.int32)


def draw_lengths(key, part):
    counts = jax.random.randint(jax.random.fold_in(key, 23), (GROUPS,), TOK_DEV // 2, TOK_DEV + 1)
    chosen = jax.random.randint(jax.random.fold_in(key, 29), (), 0, GROUPS)
    return jnp.where(jnp.arange(GROUPS, dtype=jnp.int32) == chosen, TOK_DEV, counts).astype(jnp.int32)


def steps_of(rng, shape, cuts, least, top_value):
    gain, own = 1.0, jax.random.fold_in(rng, 6)
    for dim, blocks in cuts:
        steps = jnp.exp(jax.random.uniform(jax.random.fold_in(own, dim), (blocks,), jnp.float32, least / len(cuts), top_value / len(cuts)))
        gain = gain * jnp.repeat(steps, shape[dim] // blocks).reshape([-1 if axis == dim else 1 for axis in range(len(shape))])
    return gain


def noise(rng, extent, scale, limit, cuts=(), held_as=jnp.bfloat16):
    level = steps_of(rng, extent, cuts, -0.22, 0.18) if cuts else 1.0
    array = jax.random.normal(rng, extent, jnp.float32) * scale * level
    return jnp.minimum(jnp.maximum(array, -limit), limit).astype(held_as)


def setup_inputs(seed: int = 0) -> dict:
    arg_keys = jax.random.split(jax.random.key(seed), 6)
    queries = draw_queries(jax.random.fold_in(arg_keys[5], 71), 0)
    keys = draw_keys(jax.random.fold_in(arg_keys[5], 71), 0)
    values = noise(arg_keys[2], (TOKENS, KV_HEADS * HEAD_DIM), 1.0, 6.0, ((0, 512),))
    block_mask = draw_block_mask(jax.random.fold_in(arg_keys[5], 71), 0)
    lengths = draw_lengths(jax.random.fold_in(arg_keys[5], 71), 0)
    return dict(queries=queries, keys=keys, values=values, block_mask=block_mask, lengths=lengths)


masked_score = -1.0e30


def reference(queries, keys, values, block_mask, lengths):
    per_kv = Q_HEADS // KV_HEADS
    scale = HEAD_DIM ** -0.5
    key_rows = keys.astype(jnp.float32).reshape(TOKENS, KV_HEADS, HEAD_DIM)
    value_rows = values.astype(jnp.float32).reshape(TOKENS, KV_HEADS, HEAD_DIM)
    positions = jnp.arange(TOKENS, dtype=jnp.int32)
    key_group = positions // TOK_DEV
    within = positions % TOK_DEV
    key_live = within < lengths[key_group]
    grouped = queries.reshape(GROUPS, TOK_DEV, KV_HEADS, per_kv, HEAD_DIM)

    def one_group(index):
        query_rows = grouped[index].astype(jnp.float32)
        scores = jnp.einsum("tkgd,skd->kgts", query_rows, key_rows, precision=lax.Precision.HIGHEST) * scale
        valid = key_live & (block_mask[index][key_group] > 0)
        scores = jnp.where(valid[None, None, None, :], scores, masked_score)
        top = jnp.max(scores, axis=-1, keepdims=True)
        probs = jnp.exp(scores - top)
        total = jnp.sum(probs, axis=-1)
        rounded = probs.astype(jnp.bfloat16).astype(jnp.float32)
        summed = jnp.einsum("kgts,skd->tkgd", rounded, value_rows, precision=lax.Precision.HIGHEST)
        output = summed / jnp.transpose(total, (2, 0, 1))[..., None]
        return output.astype(jnp.bfloat16).reshape(TOK_DEV, Q_HEADS * HEAD_DIM)

    result = lax.map(one_group, jnp.arange(GROUPS, dtype=jnp.int32))
    return result.reshape(TOKENS, Q_HEADS * HEAD_DIM)
```

```python
import functools
import math

import jax
import jax.numpy as jnp
from jax import lax
from jax.experimental import pallas as pl
from jax.experimental.pallas import tpu as pltpu
from jax.sharding import Mesh, PartitionSpec as P

D = 128
LOG2E = math.log2(math.e)
NEG = -1e30
NB = 512
TEAM = 4
PART = 32


def attend_kernel(me_ref, mask_ref, len_ref, q_ref, kv_ref, o_ref, kf, vf, acc, mx, sm):
    groups = mask_ref.shape[0]
    per_x = groups // TEAM
    tokens = q_ref.shape[1]
    heads = q_ref.shape[2] // D
    half = heads // 2
    rows = half * tokens
    x, rest = me_ref[0], me_ref[1]
    scale = D**-0.5 * LOG2E

    vf[...] = jnp.zeros_like(vf)

    def one_team(g, _):
        mine = g * per_x + rest

        def pack(c, off):
            j = (c // 4 % 4) * per_x + (c % 4) * 8 + c // 16
            at = pl.multiple_of(c * PART, PART)
            kf[pl.ds(off, PART), :] = kv_ref[pl.ds(at, PART), :D].astype(jnp.float32)
            vf[pl.ds(off, PART), :] = kv_ref[pl.ds(at, PART), D:].astype(jnp.float32)
            live = (len_ref[j] - x + TEAM - 1) // TEAM
            return off + jnp.where(mask_ref[mine, j] > 0, live, 0)

        count = lax.fori_loop(0, groups, pack, jnp.int32(0), unroll=8)

        acc[...] = jnp.zeros_like(acc)
        mx[...] = jnp.full_like(mx, NEG)
        sm[...] = jnp.zeros_like(sm)

        def block(b, _):
            at = pl.multiple_of(b * NB, NB)
            keys = kf[pl.ds(at, NB), :].astype(jnp.bfloat16)
            vals = vf[pl.ds(at, NB), :].astype(jnp.bfloat16)
            live = lax.broadcasted_iota(jnp.int32, (1, NB), 1) < count - at
            for part in range(2):
                r = pl.ds(part * rows, rows)
                q = jnp.concatenate(
                    [q_ref[g, :, (part * half + h) * D : (part * half + h + 1) * D] for h in range(half)], axis=0
                )
                s = lax.dot_general(q, keys, (((1,), (1,)), ((), ())), preferred_element_type=jnp.float32)
                s = jnp.where(live, s, NEG)
                old = mx[r, :]
                new = jnp.maximum(old, jnp.max(s, axis=1, keepdims=True))
                p = jnp.exp2(s * scale - (new * scale)[:, :1])
                factor = jnp.exp2((old - new) * scale)
                part_sum = p[:, :D]
                for i in range(1, NB // D):
                    part_sum = part_sum + p[:, i * D : (i + 1) * D]
                sm[r, :] = sm[r, :] * factor + part_sum
                mx[r, :] = new
                added = jnp.dot(p.astype(jnp.bfloat16), vals, preferred_element_type=jnp.float32)
                acc[r, :] = acc[r, :] * factor + added
            return 0

        lax.fori_loop(0, (count + NB - 1) // NB, block, 0)

        lane = lax.broadcasted_iota(jnp.int32, (tokens, D), 1)
        stats = jnp.zeros((tokens, D), jnp.float32)
        for h in range(heads):
            r = pl.ds(h * tokens, tokens)
            total = jnp.sum(sm[r, :], axis=1, keepdims=True)
            o_ref[g, :, h * D : (h + 1) * D] = (acc[r, :] / total).astype(jnp.bfloat16)
            lse = mx[r, :] * scale + jnp.log2(total)
            hi = lse.astype(jnp.bfloat16).astype(jnp.float32)
            mid = (lse - hi).astype(jnp.bfloat16).astype(jnp.float32)
            lo = lse - hi - mid
            stats = jnp.where(lane == h, hi, stats)
            stats = jnp.where(lane == heads + h, mid, stats)
            stats = jnp.where(lane == 2 * heads + h, lo, stats)
        o_ref[g, :, heads * D :] = stats.astype(jnp.bfloat16)
        return 0

    lax.fori_loop(0, TEAM, one_team, 0)


def combine_kernel(p_ref, o_ref):
    heads = o_ref.shape[1] // D
    stats = [p_ref[g, :, heads * D :].astype(jnp.float32) for g in range(TEAM)]
    for h in range(heads):
        lse = [
            s[:, h : h + 1] + s[:, heads + h : heads + h + 1] + s[:, 2 * heads + h : 2 * heads + h + 1] for s in stats
        ]
        top = functools.reduce(jnp.maximum, lse)
        w = [jnp.exp2(v - top) for v in lse]
        inv = 1.0 / functools.reduce(jnp.add, w)
        total = None
        for g in range(TEAM):
            term = p_ref[g, :, h * D : (h + 1) * D].astype(jnp.float32) * (w[g] * inv)
            total = term if total is None else total + term
        o_ref[:, h * D : (h + 1) * D] = total.astype(jnp.bfloat16)


VMEM = pl.BlockSpec(memory_space=pltpu.VMEM)
SMEM = pl.BlockSpec(memory_space=pltpu.SMEM)


def local(queries, keys, values, block_mask, lengths):
    groups = block_mask.shape[0]
    tokens, width = queries.shape
    heads = width // D
    x = lax.axis_index("x")
    rest = lax.axis_index(("yh", "z"))
    mine = keys.shape[0]
    kv_heads = keys.shape[1] // D
    both = jnp.stack([keys.reshape(mine // TEAM, TEAM, kv_heads, D), values.reshape(mine // TEAM, TEAM, kv_heads, D)], 3)
    both = both.transpose(1, 2, 0, 3, 4).reshape(TEAM, 1, kv_heads, mine // TEAM, 2 * D)
    both = jnp.broadcast_to(both, (TEAM, 4, kv_heads, mine // TEAM, 2 * D))
    both = both.reshape(TEAM * 4 * kv_heads, mine // TEAM, 2 * D)
    near = lax.all_to_all(both, ("x", "yh", "yl", "c"), split_axis=0, concat_axis=0, tiled=True)
    near = near.reshape(1, TEAM * 4 * PART, 2 * D)
    far = lax.all_to_all(
        jnp.broadcast_to(near, (8, TEAM * 4 * PART, 2 * D)), "z", split_axis=0, concat_axis=0, tiled=True
    )
    kv = far.reshape(groups * PART, 2 * D)
    team = lax.all_to_all(
        jnp.broadcast_to(queries[None], (TEAM, tokens, width)), "x", split_axis=0, concat_axis=0, tiled=True
    )
    me = jnp.stack([x, rest]).astype(jnp.int32)
    room = groups * PART + NB
    partial = pl.pallas_call(
        attend_kernel,
        out_shape=jax.ShapeDtypeStruct((TEAM, tokens, width + D), jnp.bfloat16),
        in_specs=[SMEM, SMEM, SMEM, VMEM, VMEM],
        out_specs=VMEM,
        scratch_shapes=[
            pltpu.VMEM((room, D), jnp.float32),
            pltpu.VMEM((room, D), jnp.float32),
            pltpu.VMEM((heads * tokens, D), jnp.float32),
            pltpu.VMEM((heads * tokens, D), jnp.float32),
            pltpu.VMEM((heads * tokens, D), jnp.float32),
        ],
        compiler_params=pltpu.CompilerParams(vmem_limit_bytes=40 * 2**20),
        name="attend",
    )(me, block_mask, lengths, team, kv)
    back = lax.all_to_all(partial, "x", split_axis=0, concat_axis=0, tiled=True)
    return pl.pallas_call(
        combine_kernel,
        out_shape=jax.ShapeDtypeStruct((tokens, width), jnp.bfloat16),
        in_specs=[VMEM],
        out_specs=VMEM,
        name="combine",
    )(back)


def solution(mesh):
    fine = Mesh(mesh.devices.reshape(4, 4, 8, 2, 2), ("x", "yh", "z", "yl", "c"))
    frames, heads = ("x", "yh", "z"), ("yl", "c")
    return jax.shard_map(
        local,
        mesh=fine,
        in_specs=(P(frames, heads), P(frames + heads, None), P(frames + heads, None), P(), P()),
        out_specs=P(frames, heads),
        check_vma=False,
    )
```

```python
import functools
import math

import jax
import jax.numpy as jnp
from jax import lax
from jax.experimental import pallas as pl
from jax.experimental.pallas import tpu as pltpu
from jax.sharding import Mesh, PartitionSpec as P


D = 128
LOG2E = math.log2(math.e)
NEG = -1e30
NB = 512
SIDE = 4
EXTRA = 16
TEAM = 4
PART = 32
VMEM = pl.BlockSpec(memory_space=pltpu.VMEM)
SMEM = pl.BlockSpec(memory_space=pltpu.SMEM)


def attend_kernel(pieces, first, last, *refs):
    me_ref, mask_ref, len_ref, q_ref = refs[:4]
    kv_refs = refs[4 : 4 + len(pieces)]
    refs = refs[4 + len(pieces) :]
    if not first:
        acc_in, mx_in, sm_in = refs[:3]
        refs = refs[3:]
    if last:
        o_ref, kf, vf, acc, mx, sm = refs
    else:
        acc_out, mx_out, sm_out, kf, vf, acc, mx, sm = refs
    groups = mask_ref.shape[0]
    per_x = groups // TEAM
    tokens = q_ref.shape[1]
    heads = q_ref.shape[2] // D
    x, rest, zb = me_ref[0], me_ref[1], me_ref[2]
    scale = D**-0.5 * LOG2E
    bias = TEAM - 1 - x
    span = SIDE * tokens

    counts = (jnp.int32(0),) * TEAM
    for kv_ref, (chunk0, chunks, shift) in zip(kv_refs, pieces):
        near = (zb + shift) & 3

        def pack(c, offs):
            j = ((c + chunk0) << 2) + near
            at = pl.multiple_of(c * PART, PART)
            key = kv_ref[pl.ds(at, PART), :D].astype(jnp.float32)
            val = kv_ref[pl.ds(at, PART), D:].astype(jnp.float32)
            live = lax.shift_right_logical(len_ref[j] + bias, 2)
            out = []
            for g in range(TEAM):
                kf[g, pl.ds(offs[g], PART), :] = key
                vf[g, pl.ds(offs[g], PART), :] = val
                out.append(offs[g] + jnp.where(mask_ref[g * per_x + rest, j] > 0, live, 0))
            return tuple(out)

        counts = lax.fori_loop(0, chunks, pack, counts, unroll=4)
    for g in range(TEAM):
        vf[g, pl.ds(counts[g], NB), :] = jnp.zeros((NB, D), jnp.float32)

    def one_team(g, _):
        count = counts[TEAM - 1]
        for i in range(TEAM - 1):
            count = jnp.where(g == i, counts[i], count)

        if first:
            acc[...] = jnp.zeros(acc.shape, jnp.float32)
            mx[...] = jnp.full(mx.shape, NEG, jnp.float32)
            sm[...] = jnp.zeros(sm.shape, jnp.float32)
        else:
            acc[...] = acc_in[g]
            mx[...] = mx_in[g]
            sm[...] = sm_in[g]

        def block(at, size, masked):
            keys = kf[g, pl.ds(at, size), :].astype(jnp.bfloat16)
            vals = vf[g, pl.ds(at, size), :].astype(jnp.bfloat16).T
            if masked:
                live = lax.broadcasted_iota(jnp.int32, (size, 1), 0) < count - at

            def scores(part):
                q = jnp.concatenate(
                    [q_ref[g, :, (part * SIDE + h) * D : (part * SIDE + h + 1) * D] for h in range(SIDE)], axis=0
                )
                s = lax.dot_general(keys, q, (((1,), (1,)), ((), ())), preferred_element_type=jnp.float32)
                return jnp.where(live, s, NEG) if masked else s

            parts = heads // SIDE
            ahead = scores(0)
            for part in range(parts):
                s = ahead
                if part + 1 < parts:
                    ahead = scores(part + 1)
                c = pl.ds(part * span, span)
                old = mx[:, c]
                new = jnp.maximum(old, jnp.max(s, axis=0, keepdims=True))
                p = jnp.exp2(s * scale - new * scale)
                factor = jnp.exp2((old - new) * scale)
                sm[:, c] = sm[:, c] * factor + jnp.sum(p, axis=0, keepdims=True)
                mx[:, c] = new
                added = jnp.dot(vals, p.astype(jnp.bfloat16), preferred_element_type=jnp.float32)
                acc[:, c] = acc[:, c] * factor + added

        full = lax.shift_right_logical(count, NB.bit_length() - 1)

        def full_block(b, _):
            block(pl.multiple_of(b * NB, NB), NB, False)
            return 0

        lax.fori_loop(0, full, full_block, 0)
        at = pl.multiple_of(full * NB, NB)

        @pl.when(count - at > NB // 2)
        def _():
            block(at, NB, True)

        @pl.when((count > at) & (count - at <= NB // 2))
        def _():
            block(at, NB // 2, True)

        if not last:
            acc_out[g] = acc[...]
            mx_out[g] = mx[...]
            sm_out[g] = sm[...]
            return 0

        total = sm[...]
        o_ref[g, :D, :] = (acc[...] * (1.0 / total)).astype(jnp.bfloat16)
        lse = mx[...] * scale + jnp.log2(total)
        hi = lse.astype(jnp.bfloat16).astype(jnp.float32)
        mid = (lse - hi).astype(jnp.bfloat16).astype(jnp.float32)
        lo = lse - hi - mid
        row = lax.broadcasted_iota(jnp.int32, (EXTRA, lse.shape[1]), 0)
        stats = jnp.where(row == 0, hi, jnp.where(row == 1, mid, jnp.where(row == 2, lo, 0.0)))
        o_ref[g, D:, :] = stats.astype(jnp.bfloat16)
        return 0

    lax.fori_loop(0, TEAM, one_team, 0)


def attend(me, block_mask, lengths, team, parts, state, last):
    tokens, width = team.shape[1:]
    rows = tokens * width // D
    pieces = tuple((chunk0, kv.shape[0] // PART, shift) for kv, chunk0, shift in parts)
    room = sum(kv.shape[0] for kv, _, _ in parts) + NB
    carried = [(D, rows), (1, rows), (1, rows)]
    if last:
        outs = jax.ShapeDtypeStruct((TEAM, D + EXTRA, rows), jnp.bfloat16)
    else:
        outs = [jax.ShapeDtypeStruct((TEAM,) + c, jnp.float32) for c in carried]
    operands = (me, block_mask, lengths, team) + tuple(kv for kv, _, _ in parts)
    aliases = {} if last else {len(operands) + i: i for i in range(len(state))}
    work = room * rows
    return pl.pallas_call(
        functools.partial(attend_kernel, pieces, not state, last),
        out_shape=outs,
        in_specs=[SMEM] * 3 + [VMEM] * (len(operands) - 3 + len(state)),
        out_specs=VMEM if last else [VMEM] * 3,
        scratch_shapes=[pltpu.VMEM((TEAM, room, D), jnp.float32)] * 2 + [pltpu.VMEM(c, jnp.float32) for c in carried],
        input_output_aliases=aliases,
        compiler_params=pltpu.CompilerParams(vmem_limit_bytes=32 * 2**20),
        cost_estimate=pl.CostEstimate(flops=8 * D * work, bytes_accessed=2**20, transcendentals=2 * work),
    )(*operands, *state)


def combine_kernel(p_ref, o_ref):
    heads = o_ref.shape[1] // D
    tokens = o_ref.shape[0]
    lse = [jnp.sum(p_ref[g, D:, :].astype(jnp.float32)[:8], axis=0, keepdims=True) for g in range(TEAM)]
    top = functools.reduce(jnp.maximum, lse)
    w = [jnp.exp2(v - top) for v in lse]
    inv = 1.0 / functools.reduce(jnp.add, w)
    w = [v * inv for v in w]
    for h in range(heads):
        c = slice(h * tokens, (h + 1) * tokens)
        total = functools.reduce(jnp.add, [p_ref[g, :D, c].astype(jnp.float32) * w[g][:, c] for g in range(TEAM)])
        o_ref[:, h * D : (h + 1) * D] = total.T.astype(jnp.bfloat16)


def stages(queries, keys, values, block_mask, lengths):
    tokens, width = queries.shape
    x = lax.axis_index("x")
    zb = lax.axis_index("zb")
    rest = lax.axis_index(("yh", "za", "zb"))
    mine = keys.shape[0]
    kv_heads = keys.shape[1] // D
    both = jnp.stack([keys.reshape(mine // TEAM, TEAM, kv_heads, D), values.reshape(mine // TEAM, TEAM, kv_heads, D)], 3)
    both = both.transpose(1, 2, 0, 3, 4).reshape(TEAM, 1, kv_heads, mine // TEAM, 2 * D)
    both = jnp.broadcast_to(both, (TEAM, 8, kv_heads, mine // TEAM, 2 * D))
    both = both.reshape(TEAM * 8 * kv_heads, mine // TEAM, 2 * D)
    own = lax.all_to_all(both, ("x", "yh", "za", "yl", "c"), split_axis=0, concat_axis=0, tiled=True)
    own = own.reshape(TEAM * 8 * PART, 2 * D)
    spread = jnp.broadcast_to(queries[None], (TEAM, tokens, width))
    team = lax.all_to_all(spread, "x", split_axis=0, concat_axis=0, tiled=True)
    up = [(i, (i + 1) % 8) for i in range(8)]
    down = [(i, (i + 7) % 8) for i in range(8)]
    half = own.shape[0] // 2
    below = lax.ppermute(own, ("za", "zb"), up)
    above = lax.ppermute(own, ("za", "zb"), down)
    far_a = lax.ppermute(above[:half], ("za", "zb"), down)
    far_b = lax.ppermute(below[half:], ("za", "zb"), up)
    me = jnp.stack([x, rest, zb]).astype(jnp.int32)
    common = (me, block_mask, lengths, team)
    state = attend(*common, [(own, 0, 0)], (), False)
    state = attend(*common, [(below, 0, 3), (above, 0, 1)], state, False)
    partial = attend(*common, [(far_a, 0, 2), (far_b, half // PART, 2)], state, True)
    back = lax.all_to_all(partial, "x", split_axis=0, concat_axis=0, tiled=True)
    return pl.pallas_call(
        combine_kernel,
        out_shape=jax.ShapeDtypeStruct((tokens, width), jnp.bfloat16),
        in_specs=[VMEM],
        out_specs=VMEM,
        name="combine",
    )(back)


def solution(mesh):
    fine = Mesh(mesh.devices.reshape(4, 4, 2, 4, 2, 2), ("x", "yh", "za", "zb", "yl", "c"))
    frames, heads = ("x", "yh", "za", "zb"), ("yl", "c")
    return jax.shard_map(
        stages,
        mesh=fine,
        in_specs=(P(frames, heads), P(frames + heads, None), P(frames + heads, None), P(), P()),
        out_specs=P(frames, heads),
        check_vma=False,
    )
```
